32 devices in a mesh: grp: 4 (over y, x), dev: 8 (over z, core).
Axes of the slice: x: 2, y: 2, z: 4, core: 2. Of those that a mesh axis runs over, the one named last changes fastest.
Arguments:
- table: float32 [262144, 128], P(('grp', 'dev')), may hold values from -6 to 6
- cold_grads: float32 [131072, 128], P(('grp', 'dev')), may hold values from -6 to 6
- cold_owner: int32 [131072, 1], P(('grp', 'dev')), may hold values from 0 to 31; in each aligned block of 4096 rows (0 to 4095, 4096 to 8191, ...) at most 256 rows name the same one
- cold_row: int32 [131072], P(('grp', 'dev')), may hold values from 0 to 8191
- hot_grads: float32 [32768, 128], P(('grp', 'dev')), may hold values from -6 to 6
- hot_slot: int32 [32768], P(('grp', 'dev')), may hold values from 0 to 255
- hot_ids: int32 [256], replicated, may hold values from 0 to 262143, as said below
Outputs:
- new_table: float32 [262144, 128], P(('grp', 'dev'))
The draws below stay inside these ranges and needn't reach their ends.
Inputs may be any that keep to these rules, and one draw needn't show every extreme that they name: `cold_owner`: among the 4096 rare-row lookups of one device no owner is named more than 256 times, a bound that some block reaches. `hot_ids`: all entries differ.
All inputs are finite; a program needn't handle non-finite values.
Results may differ from the reference program's by a relative error of at most 0.00005.
Values sent between devices are 32-bit elements; how exact they have to be, the bound alone decides.
No kernel may reach another device: no remote copies, remote signals or barrier semaphores. Data moves between devices by JAX's collectives and lax.ppermute only.
A program may use at most 64 MiB of HBM per device.

```python
import math
import jax
import jax.numpy as jnp
import numpy as np

W = 128
ROWS_DEV = 8192
HOT = 256
COLD_DEV = 4096
CAP = 256
ROWS = 262144
COLD = 131072
HOT_LOOK = 32768
DEVICES = 32


def draw_hot_ids(key, part):
    return jax.random.choice(jax.random.fold_in(key, 7), ROWS, (HOT,), replace=False).astype(jnp.int32)


def plant(array, own_key, smallest, largest):
    index_at = [jax.random.randint(jax.random.fold_in(own_key, axis), (), 0, length) for axis, length in enumerate(array.shape)]
    longest = array.shape.index(max(array.shape))
    next_to = index_at[:longest] + [(index_at[longest] + 1) % array.shape[longest]] + index_at[longest + 1:]
    return array.at[tuple(index_at)].set(smallest).at[tuple(next_to)].set(largest)


def block_scale(own_key, shape, shards, low, high):
    level = 1.0
    for axis_at, blocks in shards:
        heights = jax.random.uniform(jax.random.fold_in(jax.random.fold_in(own_key, 6), axis_at), (blocks,), jnp.float32, low / len(shards), high / len(shards))
        level = level * jnp.repeat(jnp.exp(heights), shape[axis_at] // blocks).reshape((-1,) + (1,) * (len(shape) - 1 - axis_at))
    return level


def deal_out(stream_key, own, number, rows, count, top, most, lean):
    order = jax.random.permutation(stream_key, count)
    packed, common = shares(count, rows * top, most, lean, True), shares(count, rows * top, most, lean, False)
    places = jnp.arange(count)

    def named(sizes, rotation):
        used = int((sizes > 0).sum())
        fixed = max(1, used // 4)
        moved = fixed + (places - fixed + rotation * (used - fixed)) % max(1, count - fixed)
        return jnp.zeros((count,), jnp.int32).at[order[jnp.where(places < fixed, places, moved)]].set(jnp.asarray(sizes, jnp.int32))

    sizes = jnp.where(number % 4 == 0, named(packed, number // 4), named(common, number - number // 4 - 1))
    mixed = jax.random.permutation(jax.random.fold_in(own, 3), count)
    donor, sink = mixed[0:count // 2 * 2:2], mixed[1:count // 2 * 2:2]
    room = jnp.minimum(sizes[donor] - 1, most - sizes[sink]) // 2
    room = jnp.where((donor == order[0]) | (sink == order[0]) | (sizes[sink] == 0), 0, jnp.maximum(room, 0))
    moved = jax.random.randint(jax.random.fold_in(own, 4), (count // 2,), 0, 1 << 20) % (room + 1)
    sizes = sizes.at[donor].add(-moved).at[sink].add(moved)
    members = jnp.searchsorted(jnp.cumsum(sizes), jnp.arange(rows * top), side="right").astype(jnp.int32)
    grid = members.reshape(top, rows).T
    grid = grid[jax.random.permutation(jax.random.fold_in(own, 1), rows)]
    rotation = jax.random.randint(jax.random.fold_in(own, 2), (rows, 1), 0, top)
    return jnp.take_along_axis(grid, (jnp.arange(top)[None, :] + rotation) % top, axis=1)


def shares(count, total, reach, lean, full):
    loads = [(1 << 20) // math.isqrt(grade ** lean) + 1 for grade in range(1, count + 1)]
    largest = reach if full else min(reach, max(-(-total // count), total * loads[0] // sum(loads)))
    least = 1 if total - largest >= count - 1 else 0
    holding, surplus = [largest] + [least] * (count - 1), total - largest - least * (count - 1)
    while surplus > 0:
        free = [i for i in range(1, count) if holding[i] < largest] or [i for i in range(1, count) if holding[i] < reach]
        pool, left = sum([loads[i] for i in free]), surplus
        for i in free:
            addition = min(reach - holding[i], max(1, left * loads[i] // pool), surplus)
            holding[i] = holding[i] + addition
            surplus = surplus - addition
    return np.array(holding)


def gaussian(stream_key, extent, scale, bound, split=(), kind=jnp.bfloat16):
    values = scale * jax.random.normal(stream_key, extent, jnp.float32)
    if split:
        values = values * block_scale(stream_key, extent, split, -0.22, 0.18)
    return jnp.clip(values, -bound, bound).astype(kind)


def setup_inputs(seed: int = 0) -> dict:
    key_list = jax.random.split(jax.random.key(seed), 8)
    table = gaussian(key_list[0], (ROWS, W), 1.0, 6.0, ((0, 32),), jnp.float32)
    cold_grads = gaussian(key_list[1], (COLD, W), 1.0, 6.0, ((0, 32),), jnp.float32)
    cold_owner_keys = jax.random.split(jax.random.fold_in(key_list[2], 1), COLD // COLD_DEV)
    cold_owner_turns = jax.random.permutation(jax.random.fold_in(key_list[2], 3), COLD // COLD_DEV)
    cold_owner = jax.vmap(lambda own, number: deal_out(jax.random.fold_in(key_list[2], 2), own, number, COLD_DEV, DEVICES, 1, CAP, 2))(cold_owner_keys, cold_owner_turns).reshape((COLD, 1))
    cold_row = plant(jax.random.randint(key_list[3], (COLD,), 0, ROWS_DEV), jax.random.fold_in(key_list[3], 1), 0, ROWS_DEV - 1).astype(jnp.int32)
    hot_grads = gaussian(key_list[4], (HOT_LOOK, W), 1.0, 6.0, ((0, 32),), jnp.float32)
    hot_slot = plant(jax.random.randint(key_list[5], (HOT_LOOK,), 0, HOT), jax.random.fold_in(key_list[5], 1), 0, HOT - 1).astype(jnp.int32)
    hot_ids = draw_hot_ids(jax.random.fold_in(key_list[7], 71), 0)
    return {"table": table, "cold_grads": cold_grads, "cold_owner": cold_owner, "cold_row": cold_row, "hot_grads": hot_grads, "hot_slot": hot_slot, "hot_ids": hot_ids}


def reference(table, cold_grads, cold_owner, cold_row, hot_grads, hot_slot, hot_ids):
    cold_id = (cold_owner[:, 0] * ROWS_DEV + cold_row).astype(jnp.int32)
    hot_id = hot_ids[hot_slot].astype(jnp.int32)
    new_table = table.at[cold_id].add(-0.05 * cold_grads)
    new_table = new_table.at[hot_id].add(-0.05 * hot_grads)
    return new_table
```

```python
import functools

import jax
import jax.numpy as jnp
from jax import lax
from jax.experimental import pallas as pl
from jax.experimental.pallas import tpu as pltpu
from jax.sharding import PartitionSpec as P

LEARN = 0.05
LANES = 128
UNROLL = 16
AXES = ("grp", "dev")
VMEM_LIMIT = 60000 * 1024


def copy_rows(src_ref, dst_ref, index_ref, block, slots):
    step = min(UNROLL, slots)

    def body(it, carry):
        for u in range(step):
            j = it * step + u
            dst_ref[j] = src_ref[pl.ds(index_ref[block, j], 1), :]
        return carry

    lax.fori_loop(0, slots // step, body, 0)


def pack_blocks(ks, slots, grads_ref, index_ref, ids_ref, out_refs):
    width = min(slots, LANES)
    for k, out in zip(ks, out_refs):
        copy_rows(grads_ref, out, index_ref, k, slots)
        for q in range(-(-slots // LANES)):
            out[slots + q, :, :width] = ids_ref[k : k + 1, q * LANES : q * LANES + width]


def plan_kernel(n, n_dev, slots, rows_dev, ks, owner_ref, row_ref, grads_ref, index_out, ids_out, *rest):
    outs = rest[: len(ks)]
    onehot_ref, value_ref, rank_ref, index_smem, grads_vmem, sem, sem2 = rest[len(ks) :]
    load = pltpu.make_async_copy(grads_ref, grads_vmem, sem)
    load.start()
    me = lax.axis_index("grp") * n_dev + lax.axis_index("dev")
    blocks = owner_ref.shape[0]
    owner_at = lax.broadcasted_iota(jnp.int32, (n, LANES), 0)
    slot_at = lax.broadcasted_iota(jnp.int32, (slots, LANES), 0)
    lane = lax.broadcasted_iota(jnp.int32, (1, LANES), 1)
    upper = (
        lax.broadcasted_iota(jnp.int32, (LANES, LANES), 0)
        <= lax.broadcasted_iota(jnp.int32, (LANES, LANES), 1)
    ).astype(jnp.bfloat16)
    partner = owner_ref[...] ^ me
    for r in range(blocks):
        hit = owner_at == partner[r : r + 1, :]
        onehot_ref[r * n : (r + 1) * n, :] = hit.astype(jnp.float32).astype(jnp.bfloat16)
    inclusive = jnp.dot(onehot_ref[...], upper, preferred_element_type=jnp.float32)
    base = jnp.full((n, 1), -1.0, jnp.float32)
    row1 = row_ref[...] + 1
    for r in range(blocks):
        hit = owner_at == partner[r : r + 1, :]
        counts = inclusive[r * n : (r + 1) * n, :]
        rank = jnp.sum(jnp.where(hit, counts + base, 0.0), axis=0, keepdims=True).astype(jnp.int32)
        base = base + counts[:, LANES - 1 :]
        cols = slice(r * LANES, (r + 1) * LANES)
        rank_ref[:, cols] = (slot_at == rank).astype(jnp.float32).astype(jnp.bfloat16)
        source = lane + r * LANES
        parts = (source >> 6, source & 63, row1[r : r + 1, :] >> 7, row1[r : r + 1, :] & 127)
        for p, part in enumerate(parts):
            value_ref[p * n : (p + 1) * n, cols] = jnp.where(hit, part.astype(jnp.float32), 0.0).astype(jnp.bfloat16)
    found = lax.dot_general(
        value_ref[...], rank_ref[...], (((1,), (1,)), ((), ())), preferred_element_type=jnp.float32
    )
    index = (found[:n] * 64.0 + found[n : 2 * n]).astype(jnp.int32)
    ids = found[2 * n : 3 * n] * 128.0 + found[3 * n :]
    ids_out[...] = jnp.where(ids == 0.0, float(rows_dev), ids - 1.0)
    index_out[...] = index
    to_smem = pltpu.make_async_copy(index_out, index_smem, sem2)
    to_smem.start()
    to_smem.wait()
    load.wait()
    pack_blocks(ks, slots, grads_vmem, index_smem, ids_out, outs)


def pack_kernel(slots, ks, index_ref, ids_ref, grads_ref, *outs):
    pack_blocks(ks, slots, grads_ref, index_ref, ids_ref, outs)


def plan_and_pack(n, n_dev, slots, rows_dev, first, others, owner, row, grads):
    count, width = grads.shape
    id_rows = -(-slots // LANES)
    block = jax.ShapeDtypeStruct((slots + id_rows, 1, width), jnp.float32)
    vmem = pl.BlockSpec(memory_space=pltpu.VMEM)
    params = pltpu.CompilerParams(vmem_limit_bytes=VMEM_LIMIT)
    index, ids, *first_blocks = pl.pallas_call(
        functools.partial(plan_kernel, n, n_dev, slots, rows_dev, first),
        out_shape=[
            jax.ShapeDtypeStruct((n, slots), jnp.int32),
            jax.ShapeDtypeStruct((n, slots), jnp.float32),
        ]
        + [block] * len(first),
        in_specs=[vmem, vmem, pl.BlockSpec(memory_space=pl.ANY)],
        out_specs=[vmem] * (2 + len(first)),
        scratch_shapes=[
            pltpu.VMEM((count // LANES * n, LANES), jnp.bfloat16),
            pltpu.VMEM((4 * n, count), jnp.bfloat16),
            pltpu.VMEM((slots, count), jnp.bfloat16),
            pltpu.SMEM((n, slots), jnp.int32),
            pltpu.VMEM((count, width), jnp.float32),
            pltpu.SemaphoreType.DMA,
            pltpu.SemaphoreType.DMA,
        ],
        compiler_params=params,
        name="plan",
    )(owner.reshape(count // LANES, LANES), row.reshape(count // LANES, LANES), grads)
    other_blocks = pl.pallas_call(
        functools.partial(pack_kernel, slots, others),
        out_shape=[block] * len(others),
        in_specs=[pl.BlockSpec(memory_space=pltpu.SMEM), vmem, vmem],
        out_specs=[vmem] * len(others),
        compiler_params=params,
        name="pack",
    )(index, ids, grads)
    return dict(zip(first + others, list(first_blocks) + list(other_blocks)))


def add_rows(accs, rows, row_of, id_of, count):
    ways = len(accs)
    step = min(UNROLL, count)

    def body(it, carry):
        for u0 in range(0, step, ways):
            at = [it * step + u0 + a for a in range(ways)]
            ids = [id_of(j) for j in at]
            sums = [acc[pl.ds(i, 1), :] + row_of(j) for acc, i, j in zip(accs, ids, at)]
            for acc, i, s in zip(accs, ids, sums):
                acc[pl.ds(i, 1), :] = s
        return carry

    lax.fori_loop(0, count // step, body, 0)


def apply_kernel(slots, n_blocks, n_hot, ways, *refs):
    table_ref, *refs = refs
    blocks, refs = refs[:n_blocks], refs[n_blocks:]
    hot_ids_ref = None
    hots = ()
    if n_hot:
        hot_ids_ref, *refs = refs
        hots, refs = refs[:n_hot], refs[n_hot:]
    out_ref, *refs = refs
    accs, refs = refs[:ways], refs[ways:]
    ids_vmem, ids_smem, sem = refs
    rows_dev = table_ref.shape[0]
    id_rows = -(-slots // LANES)
    for b, blk in enumerate(blocks):
        for q in range(id_rows):
            ids_vmem[b * id_rows + q : b * id_rows + q + 1, :] = blk[slots + q].astype(jnp.int32)
    to_smem = pltpu.make_async_copy(ids_vmem, ids_smem, sem)
    to_smem.start()
    chunk = 128

    def clear(it, carry):
        for acc in accs:
            acc[pl.ds(it * chunk, chunk), :] = jnp.zeros((chunk, LANES), jnp.float32)
        return carry

    lax.fori_loop(0, rows_dev // chunk, clear, 0)
    to_smem.wait()
    for b, blk in enumerate(blocks):
        for q in range(id_rows):
            add_rows(
                accs,
                None,
                lambda j, blk=blk, q=q: blk[q * LANES + j],
                lambda j, b=b, q=q: ids_smem[b * id_rows + q, j],
                min(slots, LANES),
            )
    at = 0
    for hot in hots:
        add_rows(
            accs,
            None,
            lambda j, hot=hot: hot[pl.ds(j, 1), :],
            lambda j, at=at: hot_ids_ref[at + j],
            hot.shape[0],
        )
        at += hot.shape[0]

    def combine(it, carry):
        rows = pl.ds(it * chunk, chunk)
        total = accs[0][rows, :]
        for acc in accs[1:]:
            total = total + acc[rows, :]
        out_ref[rows, :] = table_ref[rows, :] - LEARN * total
        return carry

    lax.fori_loop(0, rows_dev // chunk, combine, 0)


def apply_blocks(slots, table, blocks, hot_ids, hots, ways):
    rows_dev, width = table.shape
    id_rows = -(-slots // LANES)
    vmem = pl.BlockSpec(memory_space=pltpu.VMEM)
    smem = pl.BlockSpec(memory_space=pltpu.SMEM)
    hot_args = [hot_ids, *hots] if hots else []
    return pl.pallas_call(
        functools.partial(apply_kernel, slots, len(blocks), len(hots), ways),
        out_shape=jax.ShapeDtypeStruct(table.shape, table.dtype),
        in_specs=[vmem] * (1 + len(blocks)) + ([smem] + [vmem] * len(hots) if hots else []),
        out_specs=vmem,
        scratch_shapes=[pltpu.VMEM((rows_dev + 8, width), jnp.float32)] * ways
        + [
            pltpu.VMEM((len(blocks) * id_rows, LANES), jnp.int32),
            pltpu.SMEM((len(blocks) * id_rows, LANES), jnp.int32),
            pltpu.SemaphoreType.DMA,
        ],
        compiler_params=pltpu.CompilerParams(vmem_limit_bytes=VMEM_LIMIT),
        name="apply",
    )(table, *blocks, *hot_args)


def swap(x, axis, size, k):
    return lax.ppermute(x, axis, [(s, s ^ k) for s in range(size)])


def hot_sums(hot_grads, hot_slot, count, n_grp, n_dev):
    pick = (jnp.arange(count, dtype=jnp.int32)[:, None] == hot_slot[None, :]).astype(jnp.float32)
    partial_sum = jnp.dot(
        pick, hot_grads, precision=lax.Precision.HIGHEST, preferred_element_type=jnp.float32
    )
    part = count // n_grp
    mine = lax.axis_index("grp")
    share = lax.dynamic_slice_in_dim(partial_sum, mine * part, part, 0)
    got = [
        swap(lax.dynamic_slice_in_dim(partial_sum, (mine ^ k) * part, part, 0), "grp", n_grp, k)
        for k in range(1, n_grp)
    ]
    for g in got:
        share = share + g
    k = 1
    while k < n_dev:
        share = share + swap(share, "dev", n_dev, k)
        k *= 2
    return [share] + [swap(share, "grp", n_grp, k) for k in range(1, n_grp)]


def on_device(table, cold_grads, cold_owner, cold_row, hot_grads, hot_slot, hot_ids):
    n_grp = lax.axis_size("grp")
    n_dev = lax.axis_size("dev")
    n = n_grp * n_dev
    rows_dev = table.shape[0]
    slots = max(4, 2 * cold_grads.shape[0] // n)
    top = n_dev // 2
    cross = [k for k in range(1, n) if k & top]
    near = [k for k in range(1, n) if not k & top]
    head = max(1, len(cross) // 4)
    first, last = cross[:head], cross[-head:]
    rest = []
    middle = cross[head:-head]
    for i in range(max(len(near), len(middle))):
        rest += near[i : i + 1] + middle[i : i + 1]
    order = first + rest + last
    packed = plan_and_pack(n, n_dev, slots, rows_dev, first, rest + last + [0], cold_owner[:, 0], cold_row, cold_grads)
    got = {k: swap(packed[k], AXES, n, k) for k in order}
    got[0] = packed[0]
    hots = hot_sums(hot_grads, hot_slot, hot_ids.shape[0], n_grp, n_dev)
    local = hot_ids - lax.axis_index(AXES) * rows_dev
    target = jnp.where((local >= 0) & (local < rows_dev), local, rows_dev)
    part = hot_ids.shape[0] // n_grp
    mine = lax.axis_index("grp")
    hot_target = jnp.concatenate(
        [lax.dynamic_slice_in_dim(target, (mine ^ k) * part, part, 0) for k in range(n_grp)]
    )
    current = apply_blocks(slots, table, [got[k] for k in [0] + first + rest], hot_target, hots, 4)
    return apply_blocks(slots, current, [got[k] for k in last], None, [], 4)


def solution(mesh):
    in_specs = (
        P(AXES, None),
        P(AXES, None),
        P(AXES, None),
        P(AXES),
        P(AXES, None),
        P(AXES),
        P(),
    )
    return jax.shard_map(
        on_device, mesh=mesh, in_specs=in_specs, out_specs=P(AXES, None), check_vma=False
    )
```

```python
import functools

import jax
import jax.numpy as jnp
from jax import lax
from jax.experimental import pallas as pl
from jax.experimental.pallas import tpu as pltpu
from jax.sharding import PartitionSpec as P


LEARN = 0.05
LANES = 128
UNROLL = 32
AXES = ("grp", "dev")
MIB = 1024 * 1024
ANY = pl.BlockSpec(memory_space=pl.ANY)
VMEM = pl.BlockSpec(memory_space=pltpu.VMEM)
HBM = pl.BlockSpec(memory_space=pltpu.HBM)
SMEM = pl.BlockSpec(memory_space=pltpu.SMEM)


def in_hbm(x):
    return pltpu.with_memory_space_constraint(x, pltpu.HBM)


def id_rows_of(slots):
    return -(-slots // LANES)


def plan_kernel(n, n_dev, slots, rows_dev, ks, owner_ref, row_ref, grads_ref, index_out, ids_out, *rest):
    outs = rest[: len(ks)]
    onehot_ref, value_ref, rank_ref, index_smem, grads_vmem, owner_vmem, row_vmem, sem, sem2, sem3 = rest[len(ks) :]
    load_owner = pltpu.make_async_copy(owner_ref, owner_vmem, sem2)
    load_row = pltpu.make_async_copy(row_ref, row_vmem, sem3)
    load = pltpu.make_async_copy(grads_ref, grads_vmem, sem)
    load_owner.start()
    load_row.start()
    load.start()
    load_owner.wait()
    load_row.wait()
    me = lax.axis_index("grp") * n_dev + lax.axis_index("dev")
    blocks = owner_ref.shape[0]
    id_rows = id_rows_of(slots)
    owner_at = lax.broadcasted_iota(jnp.int32, (n, LANES), 0)
    slot_at = lax.broadcasted_iota(jnp.int32, (id_rows * LANES, LANES), 0)
    lane = lax.broadcasted_iota(jnp.int32, (1, LANES), 1)
    upper = (
        lax.broadcasted_iota(jnp.int32, (LANES, LANES), 0)
        <= lax.broadcasted_iota(jnp.int32, (LANES, LANES), 1)
    ).astype(jnp.bfloat16)
    partner = owner_vmem[...] ^ me
    for r in range(blocks):
        hit = owner_at == partner[r : r + 1, :]
        onehot_ref[r * n : (r + 1) * n, :] = hit.astype(jnp.float32).astype(jnp.bfloat16)
    inclusive = jnp.dot(onehot_ref[...], upper, preferred_element_type=jnp.float32)
    base = jnp.full((n, 1), -1.0, jnp.float32)
    row1 = row_vmem[...] + 1
    for r in range(blocks):
        hit = owner_at == partner[r : r + 1, :]
        counts = inclusive[r * n : (r + 1) * n, :]
        rank = jnp.sum(jnp.where(hit, counts + base, 0.0), axis=0, keepdims=True).astype(jnp.int32)
        base = base + counts[:, LANES - 1 :]
        cols = slice(r * LANES, (r + 1) * LANES)
        rank_ref[:, cols] = (slot_at == rank).astype(jnp.float32).astype(jnp.bfloat16)
        source = lane + r * LANES
        parts = (source >> 6, source & 63, row1[r : r + 1, :] >> 7, row1[r : r + 1, :] & 127)
        for p, part in enumerate(parts):
            value_ref[p * n : (p + 1) * n, cols] = jnp.where(hit, part.astype(jnp.float32), 0.0).astype(jnp.bfloat16)
    found = lax.dot_general(
        value_ref[...], rank_ref[...], (((1,), (1,)), ((), ())), preferred_element_type=jnp.float32
    )
    index = (found[:n] * 64.0 + found[n : 2 * n]).astype(jnp.int32)
    ids = found[2 * n : 3 * n] * 128.0 + found[3 * n :]
    ids = jnp.where(ids == 0.0, float(rows_dev), ids - 1.0)
    for q in range(id_rows):
        index_out[q * n : (q + 1) * n, :] = index[:, q * LANES : (q + 1) * LANES]
        ids_out[q * n : (q + 1) * n, :] = ids[:, q * LANES : (q + 1) * LANES]
    to_smem = pltpu.make_async_copy(index_out, index_smem, sem2)
    to_smem.start()
    to_smem.wait()
    load.wait()
    for k, out in zip(ks, outs):
        for j in range(slots):
            source_row = index_smem[j // LANES * n + k, j % LANES]
            out[j] = grads_vmem[pl.ds(source_row, 1), :]
        for q in range(id_rows):
            out[slots + q] = ids_out[q * n + k : q * n + k + 1, :]


def pack_kernel(n, slots, messages, passed, index_ref, ids_ref, grads_ref, *refs):
    passed_ref = None
    if passed:
        passed_ref, *refs = refs
    outs, refs = refs[: len(messages)], refs[len(messages) :]
    grads_vmem, *bufs, sem, pass_sem, out_sem = refs
    rows = slots + id_rows_of(slots)
    load = pltpu.make_async_copy(grads_ref, grads_vmem, sem)
    load.start()
    loads = []
    for m, parts in enumerate(messages):
        loads.append([])
        for p, (kind, i) in enumerate(parts):
            if kind == "pass":
                copy = pltpu.make_async_copy(
                    passed_ref.at[pl.ds(i * rows, rows)], bufs[m].at[pl.ds(p * rows, rows)], pass_sem.at[m]
                )
                copy.start()
                loads[m].append(copy)
    load.wait()
    step = min(UNROLL, slots)
    stores = []
    for m, parts in enumerate(messages):
        buf = bufs[m]
        for p, (kind, k) in enumerate(parts):
            if kind == "pass":
                continue
            for q in range(id_rows_of(slots)):

                def body(it, carry, q=q, k=k, base=p * rows + q * LANES):
                    for u in range(step):
                        j = it * step + u
                        source_row = index_ref[(q * n + k) * LANES + j]
                        buf[base + j] = grads_vmem[pl.ds(source_row, 1), :]
                    return carry

                lax.fori_loop(0, min(slots, LANES) // step, body, 0)
                buf[p * rows + slots + q] = ids_ref[q * n + k : q * n + k + 1, :]
        for copy in loads[m]:
            copy.wait()
        store = pltpu.make_async_copy(buf, outs[m], out_sem.at[m])
        store.start()
        stores.append(store)
    for store in stores:
        store.wait()


def block_shape(slots, width):
    return (slots + id_rows_of(slots), 1, width)


def plan(n, n_dev, slots, rows_dev, ks, owner, row, grads):
    count, width = grads.shape
    rows = id_rows_of(slots) * n
    return pl.pallas_call(
        functools.partial(plan_kernel, n, n_dev, slots, rows_dev, ks),
        out_shape=[
            jax.ShapeDtypeStruct((rows, LANES), jnp.int32),
            jax.ShapeDtypeStruct((rows, LANES), jnp.float32),
        ]
        + [jax.ShapeDtypeStruct(block_shape(slots, width), jnp.float32)] * len(ks),
        in_specs=[HBM, HBM, HBM],
        out_specs=[VMEM] * (2 + len(ks)),
        scratch_shapes=[
            pltpu.VMEM((count // LANES * n, LANES), jnp.bfloat16),
            pltpu.VMEM((4 * n, count), jnp.bfloat16),
            pltpu.VMEM((id_rows_of(slots) * LANES, count), jnp.bfloat16),
            pltpu.SMEM((rows, LANES), jnp.int32),
            pltpu.VMEM((count, width), jnp.float32),
            pltpu.VMEM((count // LANES, LANES), jnp.int32),
            pltpu.VMEM((count // LANES, LANES), jnp.int32),
            pltpu.SemaphoreType.DMA,
            pltpu.SemaphoreType.DMA,
            pltpu.SemaphoreType.DMA,
        ],
        compiler_params=pltpu.CompilerParams(vmem_limit_bytes=32 * MIB),
        name="plan",
    )(in_hbm(owner.reshape(count // LANES, LANES)), in_hbm(row.reshape(count // LANES, LANES)), in_hbm(grads))


def pack(n, slots, messages, index, ids, grads, passed=None):
    rows, one, width = block_shape(slots, grads.shape[1])
    return pl.pallas_call(
        functools.partial(pack_kernel, n, slots, messages, passed is not None),
        out_shape=[pltpu.HBM((rows * len(message), one, width), jnp.float32) for message in messages],
        in_specs=[SMEM, VMEM, HBM] + ([HBM] if passed is not None else []),
        out_specs=[HBM] * len(messages),
        scratch_shapes=[pltpu.VMEM(grads.shape, jnp.float32)]
        + [pltpu.VMEM((rows * len(message), one, width), jnp.float32) for message in messages]
        + [pltpu.SemaphoreType.DMA, pltpu.SemaphoreType.DMA((len(messages),)), pltpu.SemaphoreType.DMA((len(messages),))],
        compiler_params=pltpu.CompilerParams(vmem_limit_bytes=16 * MIB),
        name="pack",
    )(index.reshape(-1), ids, in_hbm(grads), *([passed] if passed is not None else []))


def add_rows(accs, row_of, id_of, count):
    ways = len(accs)
    step = min(UNROLL, count)

    def body(it, carry):
        for u0 in range(0, step, ways):
            at = [it * step + u0 + a for a in range(ways)]
            ids = [id_of(j) for j in at]
            sums = [acc[pl.ds(i, 1), :] - LEARN * row_of(j) for acc, i, j in zip(accs, ids, at)]
            for acc, i, s in zip(accs, ids, sums):
                acc[pl.ds(i, 1), :] = s
        return carry

    lax.fori_loop(0, count // step, body, 0)


def apply_kernel(slots, n_blocks, n_hot, ways, pieces, *refs):
    table_ref, *refs = refs
    blocks, refs = refs[:n_blocks], refs[n_blocks:]
    hot_ids_ref = None
    hots = ()
    if n_hot:
        hot_ids_ref, *refs = refs
        hots, refs = refs[:n_hot], refs[n_hot:]
    out_ref, *refs = refs
    accs, refs = refs[:ways], refs[ways:]
    ids_vmem, ids_smem, sem, table_sem, out_sem = refs
    rows_dev = table_ref.shape[0]
    id_rows = id_rows_of(slots)
    load = pltpu.make_async_copy(table_ref, accs[0].at[pl.ds(0, rows_dev)], table_sem)
    load.start()
    moves = []
    height = slots + id_rows
    parts = [(blk, base) for blk in blocks for base in range(0, blk.shape[0], height)]
    for b, (blk, base) in enumerate(parts):
        for q in range(id_rows):
            at = b * id_rows + q
            ids_vmem[at] = blk[base + slots + q].astype(jnp.int32)
            move = pltpu.make_async_copy(ids_vmem.at[at, 0], ids_smem.at[pl.ds(at * LANES, LANES)], sem)
            move.start()
            moves.append(move)
    chunk = 64

    def clear(it, carry):
        for acc in accs[1:]:
            acc[pl.ds(it * chunk, chunk), :] = jnp.zeros((chunk, LANES), jnp.float32)
        return carry

    lax.fori_loop(0, rows_dev // chunk, clear, 0)
    for move in moves:
        move.wait()
    load.wait()
    for b, (blk, base) in enumerate(parts):
        for q in range(id_rows):
            add_rows(
                accs,
                lambda j, blk=blk, base=base, q=q: blk[base + q * LANES + j],
                lambda j, at=b * id_rows + q: ids_smem[at * LANES + j],
                min(slots, LANES),
            )
    at = 0
    for hot in hots:
        add_rows(
            accs,
            lambda j, hot=hot: hot[pl.ds(j, 1), :],
            lambda j, at=at: hot_ids_ref[at + j],
            hot.shape[0],
        )
        at += hot.shape[0]
    piece = rows_dev // pieces
    stores = []
    for p in range(pieces):

        def combine(it, carry, p=p):
            rows = pl.ds(p * piece + it * chunk, chunk)
            total = accs[0][rows, :]
            for acc in accs[1:]:
                total = total + acc[rows, :]
            accs[0][rows, :] = total
            return carry

        lax.fori_loop(0, piece // chunk, combine, 0)
        rows = pl.ds(p * piece, piece)
        store = pltpu.make_async_copy(accs[0].at[rows], out_ref.at[rows], out_sem.at[p])
        store.start()
        stores.append(store)
    for store in stores:
        store.wait()


def apply_blocks(slots, table, table_spec, blocks, hot_ids, hots, ways):
    rows_dev, width = table.shape
    id_rows = id_rows_of(slots)
    hot_args = [hot_ids, *hots] if hots else []
    pieces = 8
    n_parts = sum(block.shape[0] for block in blocks) // (slots + id_rows)
    return pl.pallas_call(
        functools.partial(apply_kernel, slots, len(blocks), len(hots), ways, pieces),
        out_shape=pltpu.HBM(table.shape, table.dtype),
        in_specs=[table_spec] + [VMEM] * len(blocks) + ([SMEM] + [VMEM] * len(hots) if hots else []),
        out_specs=HBM,
        scratch_shapes=[pltpu.VMEM((rows_dev + 8, width), jnp.float32)] * ways
        + [
            pltpu.VMEM((n_parts * id_rows, 1, LANES), jnp.int32),
            pltpu.SMEM((n_parts * id_rows * LANES,), jnp.int32),
            pltpu.SemaphoreType.DMA,
            pltpu.SemaphoreType.DMA,
            pltpu.SemaphoreType.DMA((pieces,)),
        ],
        compiler_params=pltpu.CompilerParams(vmem_limit_bytes=(12 + 5 * ways) * MIB),
        name="apply",
    )(table, *blocks, *hot_args)


def swap(x, axis, size, k):
    return lax.ppermute(x, axis, [(s, s ^ k) for s in range(size)])


def scatter_share(x, axis, size, step):
    part = x.shape[0] // size
    mine = lax.axis_index(axis) // step % size
    share = lax.dynamic_slice_in_dim(x, mine * part, part, 0)
    full = lax.axis_size(axis)
    for k in range(1, size):
        share = share + swap(lax.dynamic_slice_in_dim(x, (mine ^ k) * part, part, 0), axis, full, k * step)
    return share


def partner_order(n, n_dev):
    per_grp = n_dev // 2
    near, cross = [], []
    for start in range(0, n // 2, per_grp):
        chips = range(start, start + per_grp)
        near.append([c for c in chips if c and not c & (per_grp // 2)])
        cross.append([c for c in chips if c & (per_grp // 2)])
    return near, cross


def cores_of(chips):
    return [k for c in chips for k in (2 * c, 2 * c + 1)]


def on_device(table, cold_grads, cold_owner, cold_row, hot_grads, hot_slot, hot_ids):
    n_grp = lax.axis_size("grp")
    n_dev = lax.axis_size("dev")
    n = n_grp * n_dev
    rows_dev = table.shape[0]
    hot = hot_ids.shape[0]
    slots = max(4, 2 * cold_grads.shape[0] // n)
    near, cross = partner_order(n, n_dev)
    first, second = cores_of(cross[0]), cores_of(near[1] + cross[1] + near[2])
    rest = cross[2] + near[0] + near[3] + cross[3] + [0]
    index, ids, *blocks = plan(n, n_dev, slots, rows_dev, first, cold_owner[:, 0], cold_row, cold_grads)
    blocks += pack(n, slots, [[("own", k)] for k in second], index, ids, cold_grads)
    head = []
    for k, block in zip(first + second, blocks):
        head.append(swap(block, AXES, n, k))
    (passed,) = pack(n, slots, [[("own", 2 * c + 1) for c in rest]], index, ids, cold_grads)
    passed = swap(passed, "dev", n_dev, 1)
    messages = [[("own", 2 * c), ("pass", i)] for i, c in enumerate(rest)]
    *packed, own = pack(n, slots, messages, index, ids, cold_grads, passed)
    arrived = {}
    for c, message in zip(rest, packed):
        arrived[c] = swap(message, AXES, n, 2 * c)

    pick = (jnp.arange(hot, dtype=jnp.int32)[:, None] == hot_slot[None, :]).astype(jnp.float32)
    partial_sum = jnp.dot(
        pick, hot_grads, precision=lax.Precision.HIGHEST, preferred_element_type=jnp.float32
    )
    share = scatter_share(partial_sum, "grp", n_grp, 1)
    share = scatter_share(share, "dev", 2, 1)
    whole = share
    for k in range(1, n_dev // 2):
        whole = whole + swap(share, "dev", n_dev, 2 * k)
    whole = jnp.concatenate([whole, swap(whole, "dev", n_dev, 1)])
    hots = [whole] + [swap(whole, "grp", n_grp, k) for k in range(1, n_grp)]
    local = hot_ids - lax.axis_index(AXES) * rows_dev
    target = jnp.where((local >= 0) & (local < rows_dev), local, rows_dev)
    part = hot // (2 * n_grp)
    mine = lax.axis_index("grp") * 2 + lax.axis_index("dev") % 2
    hot_target = jnp.concatenate(
        [lax.dynamic_slice_in_dim(target, (mine ^ k) * part, part, 0) for k in range(2 * n_grp)]
    )
    current = apply_blocks(slots, in_hbm(table), HBM, head + [own], None, [], 4)
    middle = [arrived[c] for c in cross[2] + near[0] + near[3]]
    current = apply_blocks(slots, in_hbm(current), HBM, middle, None, [], 4)
    return apply_blocks(slots, in_hbm(current), HBM, [arrived[c] for c in cross[3]], hot_target, hots, 2)


def solution(mesh):
    in_specs = (
        P(AXES, None),
        P(AXES, None),
        P(AXES, None),
        P(AXES),
        P(AXES, None),
        P(AXES),
        P(),
    )

    return jax.shard_map(on_device, mesh=mesh, in_specs=in_specs, out_specs=P(AXES, None), check_vma=False)
```

```python
import functools

import jax
import jax.numpy as jnp
from jax import lax
from jax.experimental import pallas as pl
from jax.experimental.pallas import tpu as pltpu
from jax.sharding import PartitionSpec as P


LEARN = 0.05
LANES = 128
UNROLL = 32
WAYS = 4
AXES = ("grp", "dev")
MIB = 1024 * 1024
ANY = pl.BlockSpec(memory_space=pl.ANY)
VMEM = pl.BlockSpec(memory_space=pltpu.VMEM)
HBM = pl.BlockSpec(memory_space=pltpu.HBM)
SMEM = pl.BlockSpec(memory_space=pltpu.SMEM)


def in_hbm(x):
    return pltpu.with_memory_space_constraint(x, pltpu.HBM)


def id_rows_of(slots):
    return -(-slots // LANES)


def plan_kernel(n, n_dev, slots, rows_dev, ks, owner_ref, row_ref, grads_ref, index_out, ids_out, *rest):
    outs = rest[: len(ks)]
    onehot_ref, value_ref, rank_ref, index_smem, grads_vmem, owner_vmem, row_vmem, sem, sem2, sem3 = rest[len(ks) :]
    load_owner = pltpu.make_async_copy(owner_ref, owner_vmem, sem2)
    load_row = pltpu.make_async_copy(row_ref, row_vmem, sem3)
    load = pltpu.make_async_copy(grads_ref, grads_vmem, sem)
    load_owner.start()
    load_row.start()
    load.start()
    load_owner.wait()
    load_row.wait()
    me = lax.axis_index("grp") * n_dev + lax.axis_index("dev")
    blocks = owner_ref.shape[0]
    id_rows = id_rows_of(slots)
    owner_at = lax.broadcasted_iota(jnp.int32, (n, LANES), 0)
    slot_at = lax.broadcasted_iota(jnp.int32, (id_rows * LANES, LANES), 0)
    lane = lax.broadcasted_iota(jnp.int32, (1, LANES), 1)
    upper = (
        lax.broadcasted_iota(jnp.int32, (LANES, LANES), 0)
        <= lax.broadcasted_iota(jnp.int32, (LANES, LANES), 1)
    ).astype(jnp.bfloat16)
    partner = owner_vmem[...] ^ me
    for r in range(blocks):
        hit = owner_at == partner[r : r + 1, :]
        onehot_ref[r * n : (r + 1) * n, :] = hit.astype(jnp.float32).astype(jnp.bfloat16)
    inclusive = jnp.dot(onehot_ref[...], upper, preferred_element_type=jnp.float32)
    base = jnp.full((n, 1), -1.0, jnp.float32)
    row1 = row_vmem[...] + 1
    for r in range(blocks):
        hit = owner_at == partner[r : r + 1, :]
        counts = inclusive[r * n : (r + 1) * n, :]
        rank = jnp.sum(jnp.where(hit, counts + base, 0.0), axis=0, keepdims=True).astype(jnp.int32)
        base = base + counts[:, LANES - 1 :]
        cols = slice(r * LANES, (r + 1) * LANES)
        rank_ref[:, cols] = (slot_at == rank).astype(jnp.float32).astype(jnp.bfloat16)
        source = lane + r * LANES
        parts = (source >> 6, source & 63, row1[r : r + 1, :] >> 7, row1[r : r + 1, :] & 127)
        for p, part in enumerate(parts):
            value_ref[p * n : (p + 1) * n, cols] = jnp.where(hit, part.astype(jnp.float32), 0.0).astype(jnp.bfloat16)
    found = lax.dot_general(
        value_ref[...], rank_ref[...], (((1,), (1,)), ((), ())), preferred_element_type=jnp.float32
    )
    index = (found[:n] * 64.0 + found[n : 2 * n]).astype(jnp.int32)
    ids = found[2 * n : 3 * n] * 128.0 + found[3 * n :]
    ids = jnp.where(ids == 0.0, float(rows_dev), ids - 1.0)
    for q in range(id_rows):
        index_out[q * n : (q + 1) * n, :] = index[:, q * LANES : (q + 1) * LANES]
        ids_out[q * n : (q + 1) * n, :] = ids[:, q * LANES : (q + 1) * LANES]
    to_smem = pltpu.make_async_copy(index_out, index_smem, sem2)
    to_smem.start()
    to_smem.wait()
    load.wait()
    for k, out in zip(ks, outs):
        for j in range(slots):
            source_row = index_smem[j // LANES * n + k, j % LANES]
            out[j] = grads_vmem[pl.ds(source_row, 1), :]
        for q in range(id_rows):
            out[slots + q] = ids_out[q * n + k : q * n + k + 1, :]


def pack_kernel(n, slots, messages, passed, index_ref, ids_ref, grads_ref, *refs):
    passed_ref = None
    if passed:
        passed_ref, *refs = refs
    outs, refs = refs[: len(messages)], refs[len(messages) :]
    grads_vmem, *bufs, sem, pass_sem, out_sem = refs
    rows = slots + id_rows_of(slots)
    load = pltpu.make_async_copy(grads_ref, grads_vmem, sem)
    load.start()
    loads = []
    for m, parts in enumerate(messages):
        loads.append([])
        for p, (kind, i) in enumerate(parts):
            if kind == "pass":
                copy = pltpu.make_async_copy(
                    passed_ref.at[pl.ds(i * rows, rows)], bufs[m].at[pl.ds(p * rows, rows)], pass_sem.at[m]
                )
                copy.start()
                loads[m].append(copy)
    load.wait()
    step = min(UNROLL, slots)
    stores = []
    for m, parts in enumerate(messages):
        buf = bufs[m]
        for p, (kind, k) in enumerate(parts):
            if kind == "pass":
                continue
            for q in range(id_rows_of(slots)):

                def body(it, carry, q=q, k=k, base=p * rows + q * LANES):
                    for u in range(step):
                        j = it * step + u
                        source_row = index_ref[(q * n + k) * LANES + j]
                        buf[base + j] = grads_vmem[pl.ds(source_row, 1), :]
                    return carry

                lax.fori_loop(0, min(slots, LANES) // step, body, 0)
                buf[p * rows + slots + q] = ids_ref[q * n + k : q * n + k + 1, :]
        for copy in loads[m]:
            copy.wait()
        store = pltpu.make_async_copy(buf, outs[m], out_sem.at[m])
        store.start()
        stores.append(store)
    for store in stores:
        store.wait()


def block_shape(slots, width):
    return (slots + id_rows_of(slots), 1, width)


def plan(n, n_dev, slots, rows_dev, ks, owner, row, grads):
    count, width = grads.shape
    rows = id_rows_of(slots) * n
    return pl.pallas_call(
        functools.partial(plan_kernel, n, n_dev, slots, rows_dev, ks),
        out_shape=[
            jax.ShapeDtypeStruct((rows, LANES), jnp.int32),
            jax.ShapeDtypeStruct((rows, LANES), jnp.float32),
        ]
        + [jax.ShapeDtypeStruct(block_shape(slots, width), jnp.float32)] * len(ks),
        in_specs=[HBM, HBM, HBM],
        out_specs=[VMEM] * (2 + len(ks)),
        scratch_shapes=[
            pltpu.VMEM((count // LANES * n, LANES), jnp.bfloat16),
            pltpu.VMEM((4 * n, count), jnp.bfloat16),
            pltpu.VMEM((id_rows_of(slots) * LANES, count), jnp.bfloat16),
            pltpu.SMEM((rows, LANES), jnp.int32),
            pltpu.VMEM((count, width), jnp.float32),
            pltpu.VMEM((count // LANES, LANES), jnp.int32),
            pltpu.VMEM((count // LANES, LANES), jnp.int32),
            pltpu.SemaphoreType.DMA,
            pltpu.SemaphoreType.DMA,
            pltpu.SemaphoreType.DMA,
        ],
        compiler_params=pltpu.CompilerParams(vmem_limit_bytes=32 * MIB),
        name="plan",
    )(in_hbm(owner.reshape(count // LANES, LANES)), in_hbm(row.reshape(count // LANES, LANES)), in_hbm(grads))


def pack(n, slots, messages, index, ids, grads, passed=None):
    rows, one, width = block_shape(slots, grads.shape[1])
    return pl.pallas_call(
        functools.partial(pack_kernel, n, slots, messages, passed is not None),
        out_shape=[pltpu.HBM((rows * len(message), one, width), jnp.float32) for message in messages],
        in_specs=[SMEM, VMEM, HBM] + ([HBM] if passed is not None else []),
        out_specs=[HBM] * len(messages),
        scratch_shapes=[pltpu.VMEM(grads.shape, jnp.float32)]
        + [pltpu.VMEM((rows * len(message), one, width), jnp.float32) for message in messages]
        + [pltpu.SemaphoreType.DMA, pltpu.SemaphoreType.DMA((len(messages),)), pltpu.SemaphoreType.DMA((len(messages),))],
        compiler_params=pltpu.CompilerParams(vmem_limit_bytes=16 * MIB),
        name="pack",
    )(index.reshape(-1), ids, in_hbm(grads), *([passed] if passed is not None else []))


def add_rows(accs, row_of, id_of, count):
    ways = len(accs)
    step = min(UNROLL, count)

    def body(it, carry):
        for u0 in range(0, step, ways):
            at = [it * step + u0 + a for a in range(ways)]
            ids = [id_of(j) for j in at]
            sums = [acc[pl.ds(i, 1), :] - LEARN * row_of(j) for acc, i, j in zip(accs, ids, at)]
            for acc, i, s in zip(accs, ids, sums):
                acc[pl.ds(i, 1), :] = s
        return carry

    lax.fori_loop(0, count // step, body, 0)


def apply_kernel(slots, n_blocks, n_hot, ways, first, last, pieces, *refs):
    table_ref = None
    if first:
        table_ref, *refs = refs
    else:
        refs = refs[ways:]
    blocks, refs = refs[:n_blocks], refs[n_blocks:]
    hot_ids_ref, hots = None, ()
    if n_hot:
        hot_ids_ref, *refs = refs
        hots, refs = refs[:n_hot], refs[n_hot:]
    accs, refs = refs[:ways], refs[ways:]
    out_ref = None
    if last:
        out_ref, *refs = refs
    ids_vmem, ids_smem, sem, table_sem, out_sem = refs
    id_rows = id_rows_of(slots)
    rows_dev = accs[0].shape[0] - 8
    if first:
        load = pltpu.make_async_copy(table_ref, accs[0].at[pl.ds(0, rows_dev)], table_sem)
        load.start()
    moves = []
    height = slots + id_rows
    parts = [(blk, base) for blk in blocks for base in range(0, blk.shape[0], height)]
    for b, (blk, base) in enumerate(parts):
        for q in range(id_rows):
            at = b * id_rows + q
            ids_vmem[at] = blk[base + slots + q].astype(jnp.int32)
            move = pltpu.make_async_copy(ids_vmem.at[at, 0], ids_smem.at[pl.ds(at * LANES, LANES)], sem)
            move.start()
            moves.append(move)
    chunk = 64
    if first:

        def clear(it, carry):
            for acc in accs[1:]:
                acc[pl.ds(it * chunk, chunk), :] = jnp.zeros((chunk, LANES), jnp.float32)
            return carry

        lax.fori_loop(0, rows_dev // chunk, clear, 0)
        load.wait()
    for move in moves:
        move.wait()
    for b, (blk, base) in enumerate(parts):
        for q in range(id_rows):
            add_rows(
                accs,
                lambda j, blk=blk, base=base, q=q: blk[base + q * LANES + j],
                lambda j, at=b * id_rows + q: ids_smem[at * LANES + j],
                min(slots, LANES),
            )
    mine = 2 * lax.axis_index("grp") + lax.axis_index("dev") % 2
    start = (lax.axis_index("grp") * lax.axis_size("dev") + lax.axis_index("dev")) * rows_dev
    for at in range(2 * n_hot):
        hot = hots[at // 2]
        part = hot.shape[0] // 2

        def target(j, base=(mine ^ at) * part):
            local = hot_ids_ref[base + j] - start
            return jnp.where((local >= 0) & (local < rows_dev), local, rows_dev)

        add_rows(accs, lambda j, hot=hot, base=at % 2 * part: hot[pl.ds(base + j, 1), :], target, part)
    if not last:
        return
    piece = rows_dev // pieces
    stores = []
    for p in range(pieces):

        def combine(it, carry, p=p):
            rows = pl.ds(p * piece + it * chunk, chunk)
            total = accs[0][rows, :]
            for acc in accs[1:]:
                total = total + acc[rows, :]
            accs[0][rows, :] = total
            return carry

        lax.fori_loop(0, piece // chunk, combine, 0)
        rows = pl.ds(p * piece, piece)
        store = pltpu.make_async_copy(accs[0].at[rows], out_ref.at[rows], out_sem.at[p])
        store.start()
        stores.append(store)
    for store in stores:
        store.wait()


def apply_blocks(slots, table, accs, blocks, hot_ids, hots, last):
    ways, pieces = WAYS, 8
    first = accs is None
    if first:
        rows_dev, width = table.shape
    else:
        rows_dev, width = accs[0].shape[0] - 8, accs[0].shape[1]
    id_rows = id_rows_of(slots)
    hot_args = [hot_ids, *hots] if hots else []
    n_parts = sum(block.shape[0] for block in blocks) // (slots + id_rows)
    outs = pl.pallas_call(
        functools.partial(apply_kernel, slots, len(blocks), len(hots), ways, first, last, pieces),
        out_shape=[pltpu.VMEM((rows_dev + 8, width), jnp.float32)] * ways
        + ([pltpu.HBM((rows_dev, width), jnp.float32)] if last else []),
        in_specs=([HBM] if first else [VMEM] * ways)
        + [VMEM] * len(blocks)
        + ([SMEM] + [VMEM] * len(hots) if hots else []),
        out_specs=[VMEM] * ways + ([HBM] if last else []),
        scratch_shapes=[
            pltpu.VMEM((n_parts * id_rows, 1, LANES), jnp.int32),
            pltpu.SMEM((n_parts * id_rows * LANES,), jnp.int32),
            pltpu.SemaphoreType.DMA,
            pltpu.SemaphoreType.DMA,
            pltpu.SemaphoreType.DMA((pieces,)),
        ],
        input_output_aliases={} if first else {w: w for w in range(ways)},
        compiler_params=pltpu.CompilerParams(vmem_limit_bytes=24 * MIB),
        name="apply",
    )(*([in_hbm(table)] if first else accs), *blocks, *hot_args)
    return outs[ways] if last else outs


def sum_kernel(*refs):
    *parts, out_ref = refs
    total = parts[0][...]
    for part in parts[1:]:
        total = total + part[...]
    out_ref[...] = total


def join_kernel(a_ref, b_ref, out_ref):
    half = a_ref.shape[0]
    out_ref[:half, :] = a_ref[...]
    out_ref[half:, :] = b_ref[...]


def small_call(kernel, shape, *args):
    return pl.pallas_call(
        kernel,
        out_shape=jax.ShapeDtypeStruct(shape, jnp.float32),
        in_specs=[VMEM] * len(args),
        out_specs=VMEM,
        compiler_params=pltpu.CompilerParams(vmem_limit_bytes=4 * MIB),
    )(*args)


def swap(x, axis, size, k):
    return lax.ppermute(x, axis, [(s, s ^ k) for s in range(size)])


def scatter_share(x, axis, size, step):
    part = x.shape[0] // size
    mine = lax.axis_index(axis) // step % size
    share = lax.dynamic_slice_in_dim(x, mine * part, part, 0)
    full = lax.axis_size(axis)
    for k in range(1, size):
        share = share + swap(lax.dynamic_slice_in_dim(x, (mine ^ k) * part, part, 0), axis, full, k * step)
    return share


def partner_order(n, n_dev):
    per_grp = n_dev // 2
    near, cross = [], []
    for start in range(0, n // 2, per_grp):
        chips = range(start, start + per_grp)
        near.append([c for c in chips if c and not c & (per_grp // 2)])
        cross.append([c for c in chips if c & (per_grp // 2)])
    return near, cross


def cores_of(chips):
    return [k for c in chips for k in (2 * c, 2 * c + 1)]


def on_device(table, cold_grads, cold_owner, cold_row, hot_grads, hot_slot, hot_ids):
    n_grp = lax.axis_size("grp")
    n_dev = lax.axis_size("dev")
    n = n_grp * n_dev
    rows_dev = table.shape[0]
    hot = hot_ids.shape[0]
    slots = max(4, 2 * cold_grads.shape[0] // n)
    near, cross = partner_order(n, n_dev)
    first, second = cores_of(cross[0]), cores_of(near[1] + cross[1] + near[2])
    rest = cross[2] + near[0] + near[3] + cross[3] + [0]
    index, ids, *blocks = plan(n, n_dev, slots, rows_dev, first, cold_owner[:, 0], cold_row, cold_grads)
    blocks += pack(n, slots, [[("own", k)] for k in second], index, ids, cold_grads)
    head = []
    for k, block in zip(first + second, blocks):
        head.append(swap(block, AXES, n, k))
    (passed,) = pack(n, slots, [[("own", 2 * c + 1) for c in rest]], index, ids, cold_grads)
    passed = swap(passed, "dev", n_dev, 1)
    messages = [[("own", 2 * c), ("pass", i)] for i, c in enumerate(rest)]
    *packed, own = pack(n, slots, messages, index, ids, cold_grads, passed)
    arrived = {}
    for c, message in zip(rest, packed):
        arrived[c] = swap(message, AXES, n, 2 * c)

    pick = (jnp.arange(hot, dtype=jnp.int32)[:, None] == hot_slot[None, :]).astype(jnp.float32)
    partial_sum = jnp.dot(
        pick, hot_grads, precision=lax.Precision.HIGHEST, preferred_element_type=jnp.float32
    )
    share = scatter_share(partial_sum, "grp", n_grp, 1)
    share = scatter_share(share, "dev", 2, 1)
    others = [swap(share, "dev", n_dev, 2 * k) for k in range(1, n_dev // 2)]
    whole = small_call(sum_kernel, share.shape, share, *others)
    other = swap(whole, "dev", n_dev, 1)
    whole = small_call(join_kernel, (2 * share.shape[0], share.shape[1]), whole, other)
    hots = [whole] + [swap(whole, "grp", n_grp, k) for k in range(1, n_grp)]
    accs = apply_blocks(slots, table, None, head + [own], None, [], False)
    accs = apply_blocks(slots, None, accs, [arrived[c] for c in near[0] + near[3]], None, [], False)
    accs = apply_blocks(slots, None, accs, [arrived[c] for c in cross[2]], None, [], False)
    accs = apply_blocks(slots, None, accs, [arrived[c] for c in cross[3][:-1]], None, [], False)
    return apply_blocks(slots, None, accs, [arrived[cross[3][-1]]], hot_ids, hots, True)


def solution(mesh):
    in_specs = (
        P(AXES, None),
        P(AXES, None),
        P(AXES, None),
        P(AXES),
        P(AXES, None),
        P(AXES),
        P(),
    )

    return jax.shard_map(on_device, mesh=mesh, in_specs=in_specs, out_specs=P(AXES, None), check_vma=False)
```

```python
import functools

import jax
import jax.numpy as jnp
from jax import lax
from jax.experimental import pallas as pl
from jax.experimental.pallas import tpu as pltpu
from jax.sharding import PartitionSpec as P


LEARN = 0.05
LANES = 128
UNROLL = 32
WAYS = 4
AXES = ("grp", "dev")
MIB = 1024 * 1024
ANY = pl.BlockSpec(memory_space=pl.ANY)
VMEM = pl.BlockSpec(memory_space=pltpu.VMEM)
HBM = pl.BlockSpec(memory_space=pltpu.HBM)
SMEM = pl.BlockSpec(memory_space=pltpu.SMEM)


def in_hbm(x):
    return pltpu.with_memory_space_constraint(x, pltpu.HBM)


def id_rows_of(slots):
    return -(-slots // LANES)


def plan_kernel(n, n_dev, slots, rows_dev, ks, owner_ref, row_ref, grads_ref, index_out, ids_out, *rest):
    outs = rest[: len(ks)]
    onehot_ref, value_ref, rank_ref, index_smem, grads_vmem, owner_vmem, row_vmem, sem, sem2, sem3 = rest[len(ks) :]
    load_owner = pltpu.make_async_copy(owner_ref, owner_vmem, sem2)
    load_row = pltpu.make_async_copy(row_ref, row_vmem, sem3)
    load = pltpu.make_async_copy(grads_ref, grads_vmem, sem)
    load_owner.start()
    load_row.start()
    load.start()
    load_owner.wait()
    me = lax.axis_index("grp") * n_dev + lax.axis_index("dev")
    blocks = owner_ref.shape[0]
    id_rows = id_rows_of(slots)
    owner_at = lax.broadcasted_iota(jnp.int32, (n, LANES), 0)
    slot_at = lax.broadcasted_iota(jnp.int32, (id_rows * LANES, LANES), 0)
    lane = lax.broadcasted_iota(jnp.int32, (1, LANES), 1)
    upper = (
        lax.broadcasted_iota(jnp.int32, (LANES, LANES), 0)
        <= lax.broadcasted_iota(jnp.int32, (LANES, LANES), 1)
    ).astype(jnp.bfloat16)
    partner = owner_vmem[...] ^ me
    for r in range(blocks):
        hit = owner_at == partner[r : r + 1, :]
        onehot_ref[r * n : (r + 1) * n, :] = hit.astype(jnp.float32).astype(jnp.bfloat16)
    inclusive = jnp.dot(onehot_ref[...], upper, preferred_element_type=jnp.float32)
    base = jnp.full((n, 1), -1.0, jnp.float32)
    load_row.wait()
    row1 = row_vmem[...] + 1
    for r in range(blocks):
        hit = owner_at == partner[r : r + 1, :]
        counts = inclusive[r * n : (r + 1) * n, :]
        rank = jnp.sum(jnp.where(hit, counts + base, 0.0), axis=0, keepdims=True).astype(jnp.int32)
        base = base + counts[:, LANES - 1 :]
        cols = slice(r * LANES, (r + 1) * LANES)
        rank_ref[:, cols] = (slot_at == rank).astype(jnp.float32).astype(jnp.bfloat16)
        source = lane + r * LANES
        parts = (source >> 6, source & 63, row1[r : r + 1, :] >> 7, row1[r : r + 1, :] & 127)
        for p, part in enumerate(parts):
            value_ref[p * n : (p + 1) * n, cols] = jnp.where(hit, part.astype(jnp.float32), 0.0).astype(jnp.bfloat16)
    found = lax.dot_general(
        value_ref[...], rank_ref[...], (((1,), (1,)), ((), ())), preferred_element_type=jnp.float32
    )
    index = (found[:n] * 64.0 + found[n : 2 * n]).astype(jnp.int32)
    ids = found[2 * n : 3 * n] * 128.0 + found[3 * n :]
    ids = jnp.where(ids == 0.0, float(rows_dev), ids - 1.0)
    for q in range(id_rows):
        index_out[q * n : (q + 1) * n, :] = index[:, q * LANES : (q + 1) * LANES]
        ids_out[q * n : (q + 1) * n, :] = ids[:, q * LANES : (q + 1) * LANES]
    low = min(ks) // 8 * 8
    count = -(-(max(ks) + 1 - low) // 8) * 8
    moves = []
    for q in range(id_rows):
        rows = pl.ds(q * n + low, count)
        moves.append(pltpu.make_async_copy(index_out.at[rows], index_smem.at[rows], sem2))
        moves[q].start()
    for move in moves:
        move.wait()
    load.wait()
    for k, out in zip(ks, outs):
        for j in range(slots):
            source_row = index_smem[j // LANES * n + k, j % LANES]
            out[j] = grads_vmem[pl.ds(source_row, 1), :]
        for q in range(id_rows):
            out[slots + q] = ids_out[q * n + k : q * n + k + 1, :]


def pack_kernel(n, slots, messages, passed, index_ref, ids_ref, grads_ref, *refs):
    passed_ref = None
    if passed:
        passed_ref, *refs = refs
    outs, refs = refs[: len(messages)], refs[len(messages) :]
    grads_vmem, *bufs, sem, pass_sem, out_sem = refs
    rows = slots + id_rows_of(slots)
    load = pltpu.make_async_copy(grads_ref, grads_vmem, sem)
    load.start()
    loads = []
    for m, parts in enumerate(messages):
        loads.append([])
        for p, (kind, i) in enumerate(parts):
            if kind == "pass":
                copy = pltpu.make_async_copy(
                    passed_ref.at[pl.ds(i * rows, rows)], bufs[m].at[pl.ds(p * rows, rows)], pass_sem.at[m]
                )
                copy.start()
                loads[m].append(copy)
    load.wait()
    step = min(UNROLL, slots)
    stores = []
    for m, parts in enumerate(messages):
        buf = bufs[m]
        for p, (kind, k) in enumerate(parts):
            if kind == "pass":
                continue
            for q in range(id_rows_of(slots)):

                def body(it, carry, q=q, k=k, base=p * rows + q * LANES):
                    for u in range(step):
                        j = it * step + u
                        source_row = index_ref[(q * n + k) * LANES + j]
                        buf[base + j] = grads_vmem[pl.ds(source_row, 1), :]
                    return carry

                lax.fori_loop(0, min(slots, LANES) // step, body, 0)
                buf[p * rows + slots + q] = ids_ref[q * n + k : q * n + k + 1, :]
        for copy in loads[m]:
            copy.wait()
        store = pltpu.make_async_copy(buf, outs[m], out_sem.at[m])
        store.start()
        stores.append(store)
    for store in stores:
        store.wait()


def block_shape(slots, width):
    return (slots + id_rows_of(slots), 1, width)


def plan(n, n_dev, slots, rows_dev, ks, owner, row, grads):
    count, width = grads.shape
    rows = id_rows_of(slots) * n
    return pl.pallas_call(
        functools.partial(plan_kernel, n, n_dev, slots, rows_dev, ks),
        out_shape=[
            jax.ShapeDtypeStruct((rows, LANES), jnp.int32),
            jax.ShapeDtypeStruct((rows, LANES), jnp.float32),
        ]
        + [jax.ShapeDtypeStruct(block_shape(slots, width), jnp.float32)] * len(ks),
        in_specs=[HBM, HBM, HBM],
        out_specs=[VMEM] * (2 + len(ks)),
        scratch_shapes=[
            pltpu.VMEM((count // LANES * n, LANES), jnp.bfloat16),
            pltpu.VMEM((4 * n, count), jnp.bfloat16),
            pltpu.VMEM((id_rows_of(slots) * LANES, count), jnp.bfloat16),
            pltpu.SMEM((rows, LANES), jnp.int32),
            pltpu.VMEM((count, width), jnp.float32),
            pltpu.VMEM((count // LANES, LANES), jnp.int32),
            pltpu.VMEM((count // LANES, LANES), jnp.int32),
            pltpu.SemaphoreType.DMA,
            pltpu.SemaphoreType.DMA,
            pltpu.SemaphoreType.DMA,
        ],
        compiler_params=pltpu.CompilerParams(vmem_limit_bytes=32 * MIB),
        name="plan",
    )(in_hbm(owner.reshape(count // LANES, LANES)), in_hbm(row.reshape(count // LANES, LANES)), in_hbm(grads))


def pack(n, slots, messages, index, ids, grads, passed=None):
    rows, one, width = block_shape(slots, grads.shape[1])
    return pl.pallas_call(
        functools.partial(pack_kernel, n, slots, messages, passed is not None),
        out_shape=[pltpu.HBM((rows * len(message), one, width), jnp.float32) for message in messages],
        in_specs=[SMEM, VMEM, HBM] + ([HBM] if passed is not None else []),
        out_specs=[HBM] * len(messages),
        scratch_shapes=[pltpu.VMEM(grads.shape, jnp.float32)]
        + [pltpu.VMEM((rows * len(message), one, width), jnp.float32) for message in messages]
        + [pltpu.SemaphoreType.DMA, pltpu.SemaphoreType.DMA((len(messages),)), pltpu.SemaphoreType.DMA((len(messages),))],
        compiler_params=pltpu.CompilerParams(vmem_limit_bytes=16 * MIB),
        name="pack",
    )(index.reshape(-1), ids, in_hbm(grads), *([passed] if passed is not None else []))


def add_rows(accs, row_of, id_of, count):
    ways = len(accs)
    step = min(UNROLL, count)

    def body(it, carry):
        for u0 in range(0, step, ways):
            at = [it * step + u0 + a for a in range(ways)]
            ids = [id_of(j) for j in at]
            sums = [acc[pl.ds(i, 1), :] - LEARN * row_of(j) for acc, i, j in zip(accs, ids, at)]
            for acc, i, s in zip(accs, ids, sums):
                acc[pl.ds(i, 1), :] = s
        return carry

    lax.fori_loop(0, count // step, body, 0)


def apply_kernel(slots, n_blocks, n_hot, ways, first, last, pieces, *refs):
    table_ref = None
    if first:
        table_ref, *refs = refs
    else:
        refs = refs[ways:]
    blocks, refs = refs[:n_blocks], refs[n_blocks:]
    hot_ids_ref, hots = None, ()
    if n_hot:
        hot_ids_ref, *refs = refs
        hots, refs = refs[:n_hot], refs[n_hot:]
    accs, refs = refs[:ways], refs[ways:]
    out_ref = None
    if last:
        out_ref, *refs = refs
    ids_vmem, ids_smem, sem, table_sem, out_sem = refs
    id_rows = id_rows_of(slots)
    rows_dev = accs[0].shape[0] - 8
    if first:
        load = pltpu.make_async_copy(table_ref, accs[0].at[pl.ds(0, rows_dev)], table_sem)
        load.start()
    moves = []
    height = slots + id_rows
    parts = [(blk, base) for blk in blocks for base in range(0, blk.shape[0], height)]
    for b, (blk, base) in enumerate(parts):
        for q in range(id_rows):
            at = b * id_rows + q
            ids_vmem[at] = blk[base + slots + q].astype(jnp.int32)
            move = pltpu.make_async_copy(ids_vmem.at[at, 0], ids_smem.at[pl.ds(at * LANES, LANES)], sem)
            move.start()
            moves.append(move)
    chunk = 64
    if first:

        def clear(it, carry):
            for acc in accs[1:]:
                acc[pl.ds(it * chunk, chunk), :] = jnp.zeros((chunk, LANES), jnp.float32)
            return carry

        lax.fori_loop(0, rows_dev // chunk, clear, 0)
        load.wait()
    for move in moves:
        move.wait()
    for b, (blk, base) in enumerate(parts):
        for q in range(id_rows):
            add_rows(
                accs,
                lambda j, blk=blk, base=base, q=q: blk[base + q * LANES + j],
                lambda j, at=b * id_rows + q: ids_smem[at * LANES + j],
                min(slots, LANES),
            )
    mine = 2 * lax.axis_index("grp") + lax.axis_index("dev") % 2
    start = (lax.axis_index("grp") * lax.axis_size("dev") + lax.axis_index("dev")) * rows_dev
    for at in range(2 * n_hot):
        hot = hots[at // 2]
        part = hot.shape[0] // 2

        def target(j, base=(mine ^ at) * part):
            local = hot_ids_ref[base + j] - start
            return jnp.where((local >= 0) & (local < rows_dev), local, rows_dev)

        add_rows(accs, lambda j, hot=hot, base=at % 2 * part: hot[pl.ds(base + j, 1), :], target, part)
    if not last:
        return
    piece = rows_dev // pieces
    stores = []
    for p in range(pieces):

        def combine(it, carry, p=p):
            rows = pl.ds(p * piece + it * chunk, chunk)
            total = accs[0][rows, :]
            for acc in accs[1:]:
                total = total + acc[rows, :]
            accs[0][rows, :] = total
            return carry

        lax.fori_loop(0, piece // chunk, combine, 0)
        rows = pl.ds(p * piece, piece)
        store = pltpu.make_async_copy(accs[0].at[rows], out_ref.at[rows], out_sem.at[p])
        store.start()
        stores.append(store)
    for store in stores:
        store.wait()


def apply_blocks(slots, table, accs, blocks, hot_ids, hots, last):
    ways, pieces = WAYS, 8
    first = accs is None
    if first:
        rows_dev, width = table.shape
    else:
        rows_dev, width = accs[0].shape[0] - 8, accs[0].shape[1]
    id_rows = id_rows_of(slots)
    hot_args = [hot_ids, *hots] if hots else []
    n_parts = sum(block.shape[0] for block in blocks) // (slots + id_rows)
    outs = pl.pallas_call(
        functools.partial(apply_kernel, slots, len(blocks), len(hots), ways, first, last, pieces),
        out_shape=[pltpu.VMEM((rows_dev + 8, width), jnp.float32)] * ways
        + ([pltpu.HBM((rows_dev, width), jnp.float32)] if last else []),
        in_specs=([HBM] if first else [VMEM] * ways)
        + [VMEM] * len(blocks)
        + ([SMEM] + [VMEM] * len(hots) if hots else []),
        out_specs=[VMEM] * ways + ([HBM] if last else []),
        scratch_shapes=[
            pltpu.VMEM((n_parts * id_rows, 1, LANES), jnp.int32),
            pltpu.SMEM((n_parts * id_rows * LANES,), jnp.int32),
            pltpu.SemaphoreType.DMA,
            pltpu.SemaphoreType.DMA,
            pltpu.SemaphoreType.DMA((pieces,)),
        ],
        input_output_aliases={} if first else {w: w for w in range(ways)},
        compiler_params=pltpu.CompilerParams(vmem_limit_bytes=24 * MIB),
        name="apply",
    )(*([in_hbm(table)] if first else accs), *blocks, *hot_args)
    return outs[ways] if last else outs


def sum_kernel(*refs):
    *parts, out_ref = refs
    total = parts[0][...]
    for part in parts[1:]:
        total = total + part[...]
    out_ref[...] = total


def join_kernel(a_ref, b_ref, out_ref):
    half = a_ref.shape[0]
    out_ref[:half, :] = a_ref[...]
    out_ref[half:, :] = b_ref[...]


def small_call(kernel, shape, *args):
    return pl.pallas_call(
        kernel,
        out_shape=jax.ShapeDtypeStruct(shape, jnp.float32),
        in_specs=[VMEM] * len(args),
        out_specs=VMEM,
        compiler_params=pltpu.CompilerParams(vmem_limit_bytes=4 * MIB),
    )(*args)


def swap(x, axis, size, k):
    return lax.ppermute(x, axis, [(s, s ^ k) for s in range(size)])


def scatter_share(x, axis, size, step):
    part = x.shape[0] // size
    mine = lax.axis_index(axis) // step % size
    share = lax.dynamic_slice_in_dim(x, mine * part, part, 0)
    full = lax.axis_size(axis)
    for k in range(1, size):
        share = share + swap(lax.dynamic_slice_in_dim(x, (mine ^ k) * part, part, 0), axis, full, k * step)
    return share


def partner_order(n, n_dev):
    per_grp = n_dev // 2
    near, cross = [], []
    for start in range(0, n // 2, per_grp):
        chips = range(start, start + per_grp)
        near.append([c for c in chips if c and not c & (per_grp // 2)])
        cross.append([c for c in chips if c & (per_grp // 2)])
    return near, cross


def cores_of(chips):
    return [k for c in chips for k in (2 * c, 2 * c + 1)]


def on_device(table, cold_grads, cold_owner, cold_row, hot_grads, hot_slot, hot_ids):
    n_grp = lax.axis_size("grp")
    n_dev = lax.axis_size("dev")
    n = n_grp * n_dev
    rows_dev = table.shape[0]
    hot = hot_ids.shape[0]
    slots = max(4, 2 * cold_grads.shape[0] // n)
    near, cross = partner_order(n, n_dev)
    first, second = cores_of(cross[0]), cores_of(near[1] + near[2] + cross[1])
    rest = cross[2] + near[0] + near[3] + cross[3] + [0]
    index, ids, *blocks = plan(n, n_dev, slots, rows_dev, first, cold_owner[:, 0], cold_row, cold_grads)
    blocks += pack(n, slots, [[("own", k)] for k in second], index, ids, cold_grads)
    head = []
    for k, block in zip(first + second, blocks):
        head.append(swap(block, AXES, n, k))
    (passed,) = pack(n, slots, [[("own", 2 * c + 1) for c in rest]], index, ids, cold_grads)
    passed = swap(passed, "dev", n_dev, 1)
    messages = [[("own", 2 * c), ("pass", i)] for i, c in enumerate(rest)]
    *packed, own = pack(n, slots, messages, index, ids, cold_grads, passed)
    arrived = {}
    for c, message in zip(rest, packed):
        arrived[c] = swap(message, AXES, n, 2 * c)

    pick = (jnp.arange(hot, dtype=jnp.int32)[:, None] == hot_slot[None, :]).astype(jnp.float32)
    partial_sum = jnp.dot(
        pick, hot_grads, precision=lax.Precision.HIGHEST, preferred_element_type=jnp.float32
    )
    share = scatter_share(partial_sum, "grp", n_grp, 1)
    share = scatter_share(share, "dev", 2, 1)
    others = [swap(share, "dev", n_dev, 2 * k) for k in range(1, n_dev // 2)]
    whole = small_call(sum_kernel, share.shape, share, *others)
    other = swap(whole, "dev", n_dev, 1)
    whole = small_call(join_kernel, (2 * share.shape[0], share.shape[1]), whole, other)
    hots = [whole] + [swap(whole, "grp", n_grp, k) for k in range(1, n_grp)]
    accs = apply_blocks(slots, table, None, head + [own], None, [], False)
    accs = apply_blocks(slots, None, accs, [arrived[c] for c in near[0] + near[3]], None, [], False)
    accs = apply_blocks(slots, None, accs, [arrived[c] for c in cross[2]], None, [], False)
    accs = apply_blocks(slots, None, accs, [arrived[c] for c in cross[3][:-1]], None, [], False)
    return apply_blocks(slots, None, accs, [arrived[cross[3][-1]]], hot_ids, hots, True)


def solution(mesh):
    in_specs = (
        P(AXES, None),
        P(AXES, None),
        P(AXES, None),
        P(AXES),
        P(AXES, None),
        P(AXES),
        P(),
    )

    return jax.shard_map(on_device, mesh=mesh, in_specs=in_specs, out_specs=P(AXES, None), check_vma=False)
```
